16 devices in a mesh: col: 2 (over z), row: 8 (over y, x, core).
Axes of the slice: x: 2, y: 2, z: 2, core: 2. Of those that a mesh axis runs over, the one named last changes fastest.
Arguments:
- t_amps: float32 [2304, 9216], P('row', 'col')
- d_denom: float32 [2304, 9216], P('row', 'col')
- v_oovv: bfloat16 [2304, 9216], P('row', 'col')
- v_vvvv: bfloat16 [9216, 9216], P('row', 'col')
- v_oooo: bfloat16 [2304, 2304], replicated
- w_mixed: bfloat16 [4608, 4608], P(None, 'col')
Outputs:
- output: float32 [2304, 9216], P('row', 'col')
All inputs are finite; a program needn't handle non-finite values.
Results may differ from the reference program's by a relative error of at most 0.00139.
Values are sent between devices in bfloat16 or wider.
A program may use at most 1 GiB of HBM per device.

```python
import jax
import jax.numpy as jnp

N_OCC = 48
N_VIR = 96
OCC_PAIRS = N_OCC * N_OCC
VIR_PAIRS = N_VIR * N_VIR
MIX_PAIRS = N_OCC * N_VIR


def setup_inputs(seed: int = 0) -> dict:
    key_list = jax.random.split(jax.random.key(seed), 6)
    t_amps = 0.4 * jax.random.normal(key_list[0], (OCC_PAIRS, VIR_PAIRS), jnp.float32)
    d_denom = jax.random.uniform(key_list[1], (OCC_PAIRS, VIR_PAIRS), jnp.float32, 1.0, 3.0)
    v_oovv = (3.75 / MIX_PAIRS) * jax.random.normal(key_list[2], (OCC_PAIRS, VIR_PAIRS), jnp.float32)
    v_vvvv = (0.75 / N_VIR) * jax.random.normal(key_list[3], (VIR_PAIRS, VIR_PAIRS), jnp.float32)
    v_oooo = (0.75 / N_OCC) * jax.random.normal(key_list[4], (OCC_PAIRS, OCC_PAIRS), jnp.float32)
    w_mixed = (0.625 * MIX_PAIRS ** -0.5) * jax.random.normal(key_list[5], (MIX_PAIRS, MIX_PAIRS), jnp.float32)
    return {
        "t_amps": t_amps,
        "d_denom": d_denom,
        "v_oovv": v_oovv.astype(jnp.bfloat16),
        "v_vvvv": v_vvvv.astype(jnp.bfloat16),
        "v_oooo": v_oooo.astype(jnp.bfloat16),
        "w_mixed": w_mixed.astype(jnp.bfloat16),
    }


def sweep_once(t_amps, d_denom, v_oovv, v_vvvv, v_oooo, w_mixed):
    t_half = t_amps.astype(jnp.bfloat16)
    ladder = jnp.dot(t_half, v_vvvv, preferred_element_type=jnp.float32)
    inter_full = jnp.dot(v_oovv, t_half.T, preferred_element_type=jnp.float32)
    hole_w = (v_oooo.astype(jnp.float32) + 0.5 * inter_full).astype(jnp.bfloat16)
    hole_term = jnp.dot(hole_w.T, t_half, preferred_element_type=jnp.float32)
    mix_in = t_half.reshape(N_OCC, N_OCC, N_VIR, N_VIR).transpose(0, 2, 1, 3).reshape(MIX_PAIRS, MIX_PAIRS)
    mix_out = jnp.dot(mix_in, w_mixed, preferred_element_type=jnp.float32)
    mix_four = mix_out.reshape(N_OCC, N_VIR, N_OCC, N_VIR).transpose(0, 2, 1, 3)
    mix_sym = (mix_four + mix_four.transpose(1, 0, 3, 2)).reshape(OCC_PAIRS, VIR_PAIRS)
    resid_sum = v_oovv.astype(jnp.float32) + ladder + hole_term + mix_sym
    return resid_sum / d_denom


def reference(t_amps, d_denom, v_oovv, v_vvvv, v_oooo, w_mixed):
    t_mid = sweep_once(t_amps, d_denom, v_oovv, v_vvvv, v_oooo, w_mixed)
    return sweep_once(t_mid, d_denom, v_oovv, v_vvvv, v_oooo, w_mixed)
```

```python
import functools
import math
import jax
import jax.numpy as jnp
from jax import lax
from jax.experimental import pallas as pl
from jax.experimental.pallas import tpu as pltpu
from jax.sharding import PartitionSpec as P


X_BIT, Y_BIT, CORE_BIT = 2, 4, 1
N_CHUNK = 3
F32 = jnp.float32
BF16 = jnp.bfloat16


def swap_row(value, bit):
    return lax.ppermute(value, "row", [(i, i ^ bit) for i in range(8)])


def swap_col(value):
    return lax.ppermute(value, "col", [(0, 1), (1, 0)])


def mm(lhs, rhs, dims=(((1,), (0,)), ((), ()))):
    return lax.dot_general(lhs, rhs, dims, preferred_element_type=F32)


def pick(flag, if_true, if_false):
    return jnp.where(flag, if_true, if_false)


def cut(value, k, size, axis):
    return lax.dynamic_slice_in_dim(value, k * size, size, axis=axis)


def split_cols(value, n):
    width = value.shape[1] // (2 * n)
    cols = [lax.slice_in_dim(value, k * width, (k + 1) * width, axis=1) for k in range(2 * n)]
    return [jnp.concatenate([cols[k], cols[n + k]], axis=1) for k in range(n)]


def join_cols(parts):
    width = parts[0].shape[1] // 2
    return jnp.concatenate([p[:, :width] for p in parts] + [p[:, width:] for p in parts], axis=1)


def order_columns(w, n_vir):
    half = n_vir // 2
    group = 8 * n_vir
    src = jnp.arange(group)
    j, rest = src // n_vir, src % n_vir
    dst = (rest // half) * (8 * half) + j * half + rest % half
    perm = (dst[:, None] == jnp.arange(group)[None, :]).astype(BF16)
    parts = [mm(lax.slice_in_dim(w, g, g + group, axis=1), perm).astype(BF16) for g in range(0, w.shape[1], group)]
    lo = [p[:, : group // 2] for p in parts]
    hi = [p[:, group // 2 :] for p in parts]
    return jnp.concatenate(lo + hi, axis=1)


def fold_kernel(occ_l, vir_l, n_occ, n_vir, pos_ref, own_ref, oth_ref, s_ref, out_ref, buf):
    half = own_ref.shape[1] // 2
    blk = occ_l * vir_l
    x, c, z = pos_ref[0], pos_ref[1], pos_ref[2]
    stride = buf.shape[0] // vir_l
    pad = jnp.zeros((vir_l, buf.shape[1] - n_vir), F32)
    for yy in range(2):
        near, far = (own_ref, oth_ref) if yy == 0 else (oth_ref, own_ref)
        for xx in range(2):
            for cc in range(2):
                s_idx = lax.bitwise_xor(x, xx) * 2 + lax.bitwise_xor(c, cc)
                for jl in range(occ_l):
                    j = ((yy * 2 + xx) * 2 + cc) * occ_l + jl
                    both = []
                    for zz in range(2):
                        m_off = zz * half + (xx * 2 + cc) * blk + jl * vir_l
                        s_off = (yy * 2 + zz) * blk + jl * vir_l
                        m = jnp.where(z == 0, near[:, m_off : m_off + vir_l], far[:, m_off : m_off + vir_l])
                        both.append(m + s_ref[s_idx, :, s_off : s_off + vir_l])
                    buf[pl.ds(j, vir_l, stride=stride), :] = jnp.concatenate(both + [pad], axis=1)
    for a in range(vir_l):
        out_ref[:, a * n_vir : (a + 1) * n_vir] = buf[a * stride : a * stride + n_occ, :n_vir]


def fold(pos, own, oth, s_all, occ_l, vir_l, n_occ, n_vir):
    width = own.shape[1]
    return pl.pallas_call(
        functools.partial(fold_kernel, occ_l, vir_l, n_occ, n_vir),
        grid=(occ_l,),
        out_shape=jax.ShapeDtypeStruct((occ_l * n_occ, vir_l * n_vir), F32),
        in_specs=[
            pl.BlockSpec(memory_space=pltpu.SMEM),
            pl.BlockSpec((vir_l, width), lambda i: (i, 0)),
            pl.BlockSpec((vir_l, width), lambda i: (i, 0)),
            pl.BlockSpec((4, vir_l, s_all.shape[2]), lambda i: (0, i, 0)),
        ],
        out_specs=pl.BlockSpec((n_occ, vir_l * n_vir), lambda i: (i, 0)),
        scratch_shapes=[pltpu.VMEM((vir_l * (n_occ + 8), 128), F32)],
        cost_estimate=pl.CostEstimate(flops=20_000_000_000, bytes_accessed=16_000_000, transcendentals=0),
        name="fold",
    )(pos, own, oth, s_all)


def ladder_kernel(pos_ref, lhs_ref, v0, v1, v2, v3, w_ref, k0, k1, k2, k3, away_ref, home_ref):
    depth = v0.shape[0]
    acc = None
    for p, v in enumerate((v0, v1, v2, v3)):
        off = pl.multiple_of(pos_ref[p] * depth, 128)
        term = jnp.dot(lhs_ref[:, pl.ds(off, depth)], v[...], preferred_element_type=F32)
        acc = term if acc is None else acc + term
    rows = k0.shape[0]
    for p, k in enumerate((k0, k1, k2, k3)):
        acc = acc + jnp.dot(w_ref[:, p * rows : (p + 1) * rows], k[...], preferred_element_type=F32)
    half = away_ref.shape[0]
    away_ref[...] = acc[:half]
    home_ref[...] = acc[half:]


def ladder(pos, lhs, v, w, k, tile):
    m, n = lhs.shape[0], v[0].shape[1]

    def full(a):
        return pl.BlockSpec(a.shape, lambda i: (0, 0), pipeline_mode=pl.Buffered(1))

    def cols(rows):
        return pl.BlockSpec((rows, tile), lambda i: (0, i))

    out = jax.ShapeDtypeStruct((m // 2, n), F32)
    return pl.pallas_call(
        ladder_kernel,
        grid=(n // tile,),
        out_shape=(out, out),
        in_specs=[pl.BlockSpec(memory_space=pltpu.SMEM), full(lhs)]
        + [cols(a.shape[0]) for a in v]
        + [full(w)]
        + [cols(a.shape[0]) for a in k],
        out_specs=(cols(m // 2), cols(m // 2)),
        cost_estimate=pl.CostEstimate(
            flops=2 * m * n * (lhs.shape[1] + w.shape[1]), bytes_accessed=24_000_000, transcendentals=0
        ),
        name="ladder",
    )(pos, lhs, *v, w, *k)


def flip_kernel(pos_ref, a0, a1, a2, a3, out_ref, buf):
    rows = a0.shape[0]
    for p, a in enumerate((a0, a1, a2, a3)):
        buf[pl.ds(pl.multiple_of(pos_ref[p] * rows, 8), rows), :] = a[...]
    out_ref[...] = buf[...].T


def flip(pos, arrays, tile):
    rows, n = arrays[0].shape
    return pl.pallas_call(
        flip_kernel,
        grid=(n // tile,),
        out_shape=jax.ShapeDtypeStruct((n, 4 * rows), F32),
        in_specs=[pl.BlockSpec(memory_space=pltpu.SMEM)] + [pl.BlockSpec((rows, tile), lambda i: (0, i))] * 4,
        out_specs=pl.BlockSpec((tile, 4 * rows), lambda i: (i, 0)),
        scratch_shapes=[pltpu.VMEM((4 * rows, tile), F32)],
        cost_estimate=pl.CostEstimate(flops=8_000_000_000, bytes_accessed=11_000_000, transcendentals=0),
        name="flip",
    )(pos, *arrays)


def finish_kernel(pos_ref, oovv_ref, home_ref, got_ref, mix_ref, d_ref, out_ref, near_ref=None):
    total = oovv_ref[...].astype(F32) + (home_ref[...] + got_ref[...]) + mix_ref[...]
    total = (total / d_ref[...]).astype(out_ref.dtype)
    out_ref[...] = total
    if near_ref is not None:

        @pl.when(pl.program_id(0) == pos_ref[0])
        def _():
            near_ref[...] = total


def finish(n, pos, oovv, home, got, mixed, d, dtype):
    rows, width = home.shape
    steps = 2
    tile = width // steps
    whole = pl.BlockSpec((rows, tile), lambda i: (0, n + N_CHUNK * i))
    part = pl.BlockSpec((rows, tile), lambda i: (0, i))
    out_shape = [jax.ShapeDtypeStruct((rows, width), dtype)]
    out_specs = [part]
    if dtype == BF16:
        out_shape.append(jax.ShapeDtypeStruct((rows, tile), dtype))
        out_specs.append(pl.BlockSpec((rows, tile), lambda i: (0, 0)))
    return pl.pallas_call(
        finish_kernel,
        grid=(steps,),
        out_shape=out_shape,
        in_specs=[pl.BlockSpec(memory_space=pltpu.SMEM), whole, part, part, whole, whole],
        out_specs=out_specs,
        cost_estimate=pl.CostEstimate(flops=3_000_000_000, bytes_accessed=9_000_000, transcendentals=0),
        name="finish",
    )(pos, oovv, home, got, mixed, d)


def mixed_product(t_four, w):
    out = jnp.einsum("ikac,kcn->ian", t_four, w, preferred_element_type=F32)
    return out.reshape(out.shape[0] * out.shape[1], -1)


def after(value, *deps):
    return lax.optimization_barrier((value, *deps))[0]


def solution(mesh):
    blk_spec = P("row", "col")

    def local_sweeps(t_block, d_block, oovv_block, vvvv_block, oooo_full, w_block):
        n_occ = math.isqrt(oooo_full.shape[0])
        n_vir = w_block.shape[0] // n_occ
        rows, cols = t_block.shape
        occ_l = n_occ // 8
        vir_l = n_vir // 2
        row = lax.axis_index("row")
        z = lax.axis_index("col")
        y, x, c = row // 4, (row // 2) % 2, row % 2
        y_is_z = y == z
        pos_fold = jnp.stack([x, c, z]).astype(jnp.int32)
        pos_ladder = jnp.stack([((y ^ dy) ^ z) * 2 + (c ^ dc) for dy, dc in ((0, 0), (1, 0), (0, 1), (1, 1))])
        pos_ladder = pos_ladder.astype(jnp.int32)

        pos_flip = jnp.stack([2 * (y ^ dy) + (z ^ dz) for dy, dz in ((0, 0), (0, 1), (1, 0), (1, 1))])
        pos_flip = pos_flip.astype(jnp.int32)

        quarter = w_block.shape[0] // 4
        piece = quarter // 2
        w_sends = [
            order_columns(lax.dynamic_slice_in_dim(w_block, (2 * x + c) * quarter + s * piece, piece, axis=0), n_vir)
            for s in range(2)
        ]
        t_first = split_cols(after(t_block, *w_sends).astype(BF16), N_CHUNK)
        w_oth = jnp.zeros(w_block.shape, BF16)
        for s in range(2):
            w_got = swap_col(w_sends[s])
            w_far = swap_row(w_got, X_BIT)
            w_q = [w_got, swap_row(w_got, CORE_BIT), w_far, swap_row(w_far, CORE_BIT)]
            for m in range(4):
                start = ((2 * x + c) ^ m) * quarter + s * piece
                w_oth = lax.dynamic_update_slice_in_dim(w_oth, w_q[m], start, axis=0)
        w_own = order_columns(after(w_block, *t_first), n_vir)
        w_own = w_own.reshape(n_occ, n_vir, w_own.shape[1])
        w_oth = w_oth.reshape(n_occ, n_vir, w_oth.shape[1])

        oovv_y = swap_row(oovv_block, Y_BIT)
        oovv_set = jnp.concatenate(
            [oovv_block, swap_row(oovv_block, CORE_BIT), oovv_y, swap_row(oovv_y, CORE_BIT)], axis=0
        )
        oooo_rows = jnp.concatenate([cut(oooo_full, row ^ m, rows, 0) for m in (0, 1, 4, 5)], axis=0)
        oooo_half = cut(oooo_rows, row ^ (X_BIT * (1 - z)), rows, 1).T.astype(F32)

        v_near = split_cols(after(vvvv_block, *t_first), N_CHUNK)
        v_set = [None] * N_CHUNK

        def fetch_v(n, part):
            part_y = swap_row(part, Y_BIT)
            v_set[n] = [part, part_y, swap_row(part, CORE_BIT), swap_row(part_y, CORE_BIT)]

        def near_half(p):
            wide = p.shape[1] // 2
            return pick(x == 0, p[:, :wide], p[:, wide:])

        def sweep(t_parts, near_parts, last):
            t_x = [swap_row(p, X_BIT) for p in t_parts]
            t_y = [swap_row(p, Y_BIT) for p in t_parts]
            t_c = [swap_row(p, CORE_BIT) for p in t_parts]
            t_yc = [swap_row(p, CORE_BIT) for p in t_y]
            t_full = join_cols(t_parts)
            tx_full = join_cols(t_x)

            def far(send):
                return jnp.concatenate([swap_col(p) for p in send], axis=1)

            t_rows = jnp.concatenate([tx_full, t_full], axis=0)
            if not last:
                for n in range(N_CHUNK - 1):
                    fetch_v(n, v_near[n])

            t_four = t_full.reshape(occ_l, n_occ, vir_l, n_vir)
            mix_own = mixed_product(t_four, w_own)
            far_own = far(near_parts)

            if last:
                mix_oth = mixed_product(t_four, w_oth)
                t_rows = after(t_rows, mix_oth)
            inter = mm(t_rows, oovv_set, (((1,), (1,)), ((), ())))
            inter_send = cut(inter, 1 - z, rows, 0)
            inter_sum = cut(inter, z, rows, 0) + swap_col(inter_send)
            hole_half = (oooo_half + 0.5 * inter_sum).astype(BF16)
            hole_got = swap_col(hole_half)
            hole_w = jnp.concatenate([pick(z == 0, hole_half, hole_got), pick(z == 0, hole_got, hole_half)], axis=0)

            near_x = [near_half(p) for p in t_x[:-1]]
            near_x.append(near_half(after(t_x[-1], *near_x)))
            far_x = far(near_x)
            near = cut(t_rows, x, cols // 2, 1)
            lhs = jnp.concatenate([near, jnp.concatenate([far_x, far_own], axis=0)], axis=1)

            if not last:
                t_late = after(t_four, hole_half)
                mix_oth = mixed_product(t_late, w_oth)

            half_w = mix_own.shape[1] // 2
            keep_own, keep_oth = cut(mix_own, z, half_w, 1), cut(mix_oth, z, half_w, 1)
            give_own, give_oth = cut(mix_own, 1 - z, half_w, 1), cut(mix_oth, 1 - z, half_w, 1)
            got_away = swap_col(pick(y_is_z, give_oth, give_own))
            got_here = swap_col(pick(y_is_z, give_own, give_oth))
            send0 = pick(y_is_z, keep_oth, keep_own)

            def ladder_part(n):
                k_rows = (t_parts[n], t_c[n], t_y[n], t_yc[n])
                away, home = ladder(pos_ladder, lhs, v_set[n], hole_w, k_rows, 512)
                return away, home, swap_row(away, X_BIT)

            here = pick(y_is_z, keep_own, keep_oth)
            away0, away1 = swap_row(send0, Y_BIT), swap_row(got_away, Y_BIT)
            terms = [None] * N_CHUNK
            if not last:
                fetch_v(N_CHUNK - 1, after(v_near[-1], send0, got_away))
                for n in range(N_CHUNK - 1):
                    terms[n] = ladder_part(n)
                here = after(here, *[t[0] for t in terms[:-1]])
            flipped = flip(pos_flip, (here, got_here, away0, away1), 384)
            by_x = [cut(flipped, x, 2 * rows, 0), swap_row(cut(flipped, 1 - x, 2 * rows, 0), X_BIT)]
            s_all = []
            for f in by_x:
                s_all += [cut(f, c, rows, 0), swap_row(cut(f, 1 - c, rows, 0), CORE_BIT)]
            s_all = jnp.stack(s_all)
            mixed = fold(pos_fold, mix_own, mix_oth, s_all, occ_l, vir_l, n_occ, n_vir)

            def close(n):
                _, home, got = terms[n]
                return finish(n, pos_fold, oovv_block, home, got, mixed, d_block, F32 if last else BF16)

            for n in range(N_CHUNK):
                if terms[n] is None:
                    terms[n] = ladder_part(n)
            return [close(n) for n in range(N_CHUNK)]

        mid = sweep(t_first, [near_half(p) for p in t_first], False)
        final = sweep([p[0] for p in mid], [p[1] for p in mid], True)
        return join_cols([p[0] for p in final])

    return jax.shard_map(
        local_sweeps,
        mesh=mesh,
        in_specs=(blk_spec, blk_spec, blk_spec, blk_spec, P(), P(None, "col")),
        out_specs=blk_spec,
        check_vma=False,
    )
```

```python
import functools
import math
import jax
import jax.numpy as jnp
from jax import lax
from jax.experimental import pallas as pl
from jax.experimental.pallas import tpu as pltpu
from jax.sharding import PartitionSpec as P


X_BIT, Y_BIT, CORE_BIT = 2, 4, 1
N_CHUNK = 3
F32 = jnp.float32
BF16 = jnp.bfloat16


def swap_row(value, bit):
    return lax.ppermute(value, "row", [(i, i ^ bit) for i in range(8)])


def swap_col(value):
    return lax.ppermute(value, "col", [(0, 1), (1, 0)])


def mm(lhs, rhs, dims=(((1,), (0,)), ((), ()))):
    return lax.dot_general(lhs, rhs, dims, preferred_element_type=F32)


def pick(flag, if_true, if_false):
    return jnp.where(flag, if_true, if_false)


def cut(value, k, size, axis):
    return lax.dynamic_slice_in_dim(value, k * size, size, axis=axis)


def split_cols(value, n):
    width = value.shape[1] // (2 * n)
    cols = [lax.slice_in_dim(value, k * width, (k + 1) * width, axis=1) for k in range(2 * n)]
    return [jnp.concatenate([cols[k], cols[n + k]], axis=1) for k in range(n)]


def join_cols(parts):
    width = parts[0].shape[1] // 2
    return jnp.concatenate([p[:, :width] for p in parts] + [p[:, width:] for p in parts], axis=1)


def order_kernel(w_ref, perm_ref, out_ref):
    group = perm_ref.shape[0]
    half = w_ref.shape[1] // 2
    for g in range(w_ref.shape[1] // group):
        moved = jnp.dot(w_ref[:, g * group : (g + 1) * group], perm_ref[...], preferred_element_type=F32).astype(BF16)
        out_ref[:, g * (group // 2) : (g + 1) * (group // 2)] = moved[:, : group // 2]
        out_ref[:, half + g * (group // 2) : half + (g + 1) * (group // 2)] = moved[:, group // 2 :]


def order_columns(w, n_vir):
    half = n_vir // 2
    group = 8 * n_vir
    src = jnp.arange(group)
    j, rest = src // n_vir, src % n_vir
    dst = (rest // half) * (8 * half) + j * half + rest % half
    perm = (dst[:, None] == jnp.arange(group)[None, :]).astype(BF16)
    tile = 288
    block = pl.BlockSpec((tile, w.shape[1]), lambda i: (i, 0))
    return pl.pallas_call(
        order_kernel,
        grid=(w.shape[0] // tile,),
        out_shape=jax.ShapeDtypeStruct(w.shape, BF16),
        in_specs=[block, pl.BlockSpec(perm.shape, lambda i: (0, 0))],
        out_specs=block,
        cost_estimate=pl.CostEstimate(
            flops=2 * w.size * group, bytes_accessed=4 * w.size, transcendentals=0
        ),
        name="order",
    )(w, perm)


def fold_kernel(occ_l, vir_l, n_occ, n_vir, pos_ref, own_ref, oth_ref, s_ref, out_ref, buf):
    half = own_ref.shape[1] // 2
    blk = occ_l * vir_l
    x, c, z = pos_ref[0], pos_ref[1], pos_ref[2]
    stride = buf.shape[0] // vir_l
    pad = jnp.zeros((vir_l, buf.shape[1] - n_vir), F32)
    for yy in range(2):
        near, far = (own_ref, oth_ref) if yy == 0 else (oth_ref, own_ref)
        for xx in range(2):
            for cc in range(2):
                s_idx = lax.bitwise_xor(x, xx) * 2 + lax.bitwise_xor(c, cc)
                for jl in range(occ_l):
                    j = ((yy * 2 + xx) * 2 + cc) * occ_l + jl
                    both = []
                    for zz in range(2):
                        m_off = zz * half + (xx * 2 + cc) * blk + jl * vir_l
                        s_off = (yy * 2 + zz) * blk + jl * vir_l
                        m = jnp.where(z == 0, near[:, m_off : m_off + vir_l], far[:, m_off : m_off + vir_l])
                        both.append(m + s_ref[s_idx, :, s_off : s_off + vir_l])
                    buf[pl.ds(j, vir_l, stride=stride), :] = jnp.concatenate(both + [pad], axis=1)
    for a in range(vir_l):
        out_ref[:, a * n_vir : (a + 1) * n_vir] = buf[a * stride : a * stride + n_occ, :n_vir]


def fold(pos, own, oth, s_all, occ_l, vir_l, n_occ, n_vir):
    width = own.shape[1]
    return pl.pallas_call(
        functools.partial(fold_kernel, occ_l, vir_l, n_occ, n_vir),
        grid=(occ_l,),
        out_shape=jax.ShapeDtypeStruct((occ_l * n_occ, vir_l * n_vir), F32),
        in_specs=[
            pl.BlockSpec(memory_space=pltpu.SMEM),
            pl.BlockSpec((vir_l, width), lambda i: (i, 0)),
            pl.BlockSpec((vir_l, width), lambda i: (i, 0)),
            pl.BlockSpec((4, vir_l, s_all.shape[2]), lambda i: (0, i, 0)),
        ],
        out_specs=pl.BlockSpec((n_occ, vir_l * n_vir), lambda i: (i, 0)),
        scratch_shapes=[pltpu.VMEM((vir_l * (n_occ + 8), 128), F32)],
        cost_estimate=pl.CostEstimate(flops=20_000_000_000, bytes_accessed=16_000_000, transcendentals=0),
        name="fold",
    )(pos, own, oth, s_all)


def ladder_kernel(pos_ref, t_ref, *refs):
    *far, v0, v1, v2, v3, w_ref, k0, k1, k2, k3, away_ref, home_ref, lhs_ref = refs
    depth = v0.shape[0]

    @pl.when(pl.program_id(0) == 0)
    def _():
        near = t_ref.shape[1] // 2
        lhs_ref[:, :near] = t_ref[:, pl.ds(pl.multiple_of(pos_ref[4] * near, 128), near)]
        rows, wide = far[0].shape
        count = len(far) // 2
        for n in range(count):
            lhs_ref[:rows, near + n * wide : near + (n + 1) * wide] = far[n][...]
            lhs_ref[rows:, near + n * wide : near + (n + 1) * wide] = far[count + n][...]

    acc = None
    for p, v in enumerate((v0, v1, v2, v3)):
        off = pl.multiple_of(pos_ref[p] * depth, 128)
        term = jnp.dot(lhs_ref[:, pl.ds(off, depth)], v[...], preferred_element_type=F32)
        acc = term if acc is None else acc + term
    rows = k0.shape[0]
    for p, k in enumerate((k0, k1, k2, k3)):
        acc = acc + jnp.dot(w_ref[:, p * rows : (p + 1) * rows], k[...], preferred_element_type=F32)
    half = away_ref.shape[0]
    away_ref[...] = acc[:half]
    home_ref[...] = acc[half:]


def ladder(pos, t_rows, far, v, w, k, tile):
    m, n = t_rows.shape[0], v[0].shape[1]

    def full(a):
        return pl.BlockSpec(a.shape, lambda i: (0, 0), pipeline_mode=pl.Buffered(1))

    def cols(rows):
        return pl.BlockSpec((rows, tile), lambda i: (0, i))

    out = jax.ShapeDtypeStruct((m // 2, n), F32)
    return pl.pallas_call(
        ladder_kernel,
        grid=(n // tile,),
        out_shape=(out, out),
        in_specs=[pl.BlockSpec(memory_space=pltpu.SMEM), full(t_rows)]
        + [full(a) for a in far]
        + [cols(a.shape[0]) for a in v]
        + [full(w)]
        + [cols(a.shape[0]) for a in k],
        out_specs=(cols(m // 2), cols(m // 2)),
        scratch_shapes=[pltpu.VMEM(t_rows.shape, BF16)],
        cost_estimate=pl.CostEstimate(
            flops=2 * m * n * (t_rows.shape[1] + w.shape[1]), bytes_accessed=24_000_000, transcendentals=0
        ),
        name="ladder",
    )(pos, t_rows, *far, *v, w, *k)


def flip_kernel(pos_ref, a0, a1, a2, a3, out_ref, buf):
    rows = a0.shape[0]
    for p, a in enumerate((a0, a1, a2, a3)):
        buf[pl.ds(pl.multiple_of(pos_ref[p] * rows, 8), rows), :] = a[...]
    out_ref[...] = buf[...].T


def flip(pos, arrays, tile):
    rows, n = arrays[0].shape
    return pl.pallas_call(
        flip_kernel,
        grid=(n // tile,),
        out_shape=jax.ShapeDtypeStruct((n, 4 * rows), F32),
        in_specs=[pl.BlockSpec(memory_space=pltpu.SMEM)] + [pl.BlockSpec((rows, tile), lambda i: (0, i))] * 4,
        out_specs=pl.BlockSpec((tile, 4 * rows), lambda i: (i, 0)),
        scratch_shapes=[pltpu.VMEM((4 * rows, tile), F32)],
        cost_estimate=pl.CostEstimate(flops=8_000_000_000, bytes_accessed=11_000_000, transcendentals=0),
        name="flip",
    )(pos, *arrays)


def finish_kernel(pos_ref, oovv_ref, home_ref, got_ref, mix_ref, d_ref, out_ref, near_ref=None):
    total = oovv_ref[...].astype(F32) + (home_ref[...] + got_ref[...]) + mix_ref[...]
    total = (total / d_ref[...]).astype(out_ref.dtype)
    out_ref[...] = total
    if near_ref is not None:

        @pl.when(pl.program_id(0) == pos_ref[0])
        def _():
            near_ref[...] = total


def finish(n, pos, oovv, home, got, mixed, d, dtype):
    rows, width = home.shape
    steps = 2
    tile = width // steps
    whole = pl.BlockSpec((rows, tile), lambda i: (0, n + N_CHUNK * i))
    part = pl.BlockSpec((rows, tile), lambda i: (0, i))
    out_shape = [jax.ShapeDtypeStruct((rows, width), dtype)]
    out_specs = [part]
    if dtype == BF16:
        out_shape.append(jax.ShapeDtypeStruct((rows, tile), dtype))
        out_specs.append(pl.BlockSpec((rows, tile), lambda i: (0, 0)))
    return pl.pallas_call(
        finish_kernel,
        grid=(steps,),
        out_shape=out_shape,
        in_specs=[pl.BlockSpec(memory_space=pltpu.SMEM), whole, part, part, whole, whole],
        out_specs=out_specs,
        cost_estimate=pl.CostEstimate(flops=3_000_000_000, bytes_accessed=9_000_000, transcendentals=0),
        name="finish",
    )(pos, oovv, home, got, mixed, d)


def mixed_product(t_four, w):
    out = jnp.einsum("ikac,kcn->ian", t_four, w, preferred_element_type=F32)
    return out.reshape(out.shape[0] * out.shape[1], -1)


def after(value, *deps):
    return lax.optimization_barrier((value, *deps))[0]


def solution(mesh):
    blk_spec = P("row", "col")

    def local_sweeps(t_block, d_block, oovv_block, vvvv_block, oooo_full, w_block):
        n_occ = math.isqrt(oooo_full.shape[0])
        n_vir = w_block.shape[0] // n_occ
        rows, _ = t_block.shape
        occ_l = n_occ // 8
        vir_l = n_vir // 2
        row = lax.axis_index("row")
        z = lax.axis_index("col")
        y, x, c = row // 4, (row // 2) % 2, row % 2
        y_is_z = y == z
        pos_fold = jnp.stack([x, c, z]).astype(jnp.int32)
        pos_ladder = jnp.stack([((y ^ dy) ^ z) * 2 + (c ^ dc) for dy, dc in ((0, 0), (1, 0), (0, 1), (1, 1))] + [x])
        pos_ladder = pos_ladder.astype(jnp.int32)

        pos_flip = jnp.stack([2 * (y ^ dy) + (z ^ dz) for dy, dz in ((0, 0), (0, 1), (1, 0), (1, 1))])
        pos_flip = pos_flip.astype(jnp.int32)

        quarter = w_block.shape[0] // 4
        piece = quarter // 2
        w_sends = [
            order_columns(lax.dynamic_slice_in_dim(w_block, (2 * x + c) * quarter + s * piece, piece, axis=0), n_vir)
            for s in range(2)
        ]
        t_first = split_cols(after(t_block, *w_sends).astype(BF16), N_CHUNK)
        w_list, w_starts = [], []
        for s in range(2):
            w_got = swap_col(w_sends[s])
            w_far = swap_row(w_got, X_BIT)
            w_q = [w_got, swap_row(w_got, CORE_BIT), w_far, swap_row(w_far, CORE_BIT)]
            for m in range(4):
                w_starts.append((((2 * x + c) ^ m) * quarter + s * piece) // n_vir)
                w_list.append(w_q[m])
        w_oth = jnp.concatenate(w_list, axis=0)
        n_list = piece // n_vir
        w_own = order_columns(after(w_block, *t_first), n_vir)
        w_own = w_own.reshape(n_occ, n_vir, w_own.shape[1])
        w_oth = w_oth.reshape(n_occ, n_vir, w_oth.shape[1])

        oovv_y = swap_row(oovv_block, Y_BIT)
        oovv_set = jnp.concatenate(
            [oovv_block, swap_row(oovv_block, CORE_BIT), oovv_y, swap_row(oovv_y, CORE_BIT)], axis=0
        )
        oooo_rows = jnp.concatenate([cut(oooo_full, row ^ m, rows, 0) for m in (0, 1, 4, 5)], axis=0)
        oooo_half = cut(oooo_rows, row ^ (X_BIT * (1 - z)), rows, 1).T.astype(F32)

        v_near = split_cols(after(vvvv_block, *t_first), N_CHUNK)
        v_set = [None] * N_CHUNK

        def fetch_v(n, part):
            part_y = swap_row(part, Y_BIT)
            v_set[n] = [part, part_y, swap_row(part, CORE_BIT), swap_row(part_y, CORE_BIT)]

        def near_half(p):
            wide = p.shape[1] // 2
            return pick(x == 0, p[:, :wide], p[:, wide:])

        def sweep(t_parts, near_parts, last):
            t_x = [swap_row(p, X_BIT) for p in t_parts]
            t_y = [swap_row(p, Y_BIT) for p in t_parts]
            t_c = [swap_row(p, CORE_BIT) for p in t_parts]
            t_yc = [swap_row(p, CORE_BIT) for p in t_y]
            t_full = join_cols(t_parts)
            tx_full = join_cols(t_x)

            def far(send):
                return [swap_col(p) for p in send]

            t_rows = jnp.concatenate([tx_full, t_full], axis=0)
            if not last:
                for n in range(N_CHUNK - 1):
                    fetch_v(n, v_near[n])

            t_four = t_full.reshape(occ_l, n_occ, vir_l, n_vir)
            t_oth = jnp.concatenate([lax.dynamic_slice_in_dim(t_four, k, n_list, axis=1) for k in w_starts], axis=1)
            mix_own = mixed_product(t_four, w_own)
            far_own = far(near_parts)

            if last:
                mix_oth = mixed_product(t_oth, w_oth)
                t_rows = after(t_rows, mix_oth)
            inter = mm(t_rows, oovv_set, (((1,), (1,)), ((), ())))
            inter_send = cut(inter, 1 - z, rows, 0)
            inter_sum = cut(inter, z, rows, 0) + swap_col(inter_send)
            hole_half = (oooo_half + 0.5 * inter_sum).astype(BF16)
            hole_got = swap_col(hole_half)
            hole_w = jnp.concatenate([pick(z == 0, hole_half, hole_got), pick(z == 0, hole_got, hole_half)], axis=0)

            near_x = [near_half(p) for p in t_x[:-1]]
            near_x.append(near_half(after(t_x[-1], *near_x)))
            far_x = far(near_x)

            if not last:
                t_late = after(t_oth, hole_half)
                mix_oth = mixed_product(t_late, w_oth)

            half_w = mix_own.shape[1] // 2
            keep_own, keep_oth = cut(mix_own, z, half_w, 1), cut(mix_oth, z, half_w, 1)
            give_own, give_oth = cut(mix_own, 1 - z, half_w, 1), cut(mix_oth, 1 - z, half_w, 1)
            got_away = swap_col(pick(y_is_z, give_oth, give_own))
            got_here = swap_col(pick(y_is_z, give_own, give_oth))
            send0 = pick(y_is_z, keep_oth, keep_own)

            def ladder_part(n):
                k_rows = (t_parts[n], t_c[n], t_y[n], t_yc[n])
                away, home = ladder(pos_ladder, t_rows, far_x + far_own, v_set[n], hole_w, k_rows, 256)
                return away, home, swap_row(away, X_BIT)

            here = pick(y_is_z, keep_own, keep_oth)
            away0, away1 = swap_row(send0, Y_BIT), swap_row(got_away, Y_BIT)
            terms = [None] * N_CHUNK
            if not last:
                fetch_v(N_CHUNK - 1, after(v_near[-1], send0, got_away))
                for n in range(N_CHUNK - 1):
                    terms[n] = ladder_part(n)
                here = after(here, *[t[0] for t in terms[:-1]])
            flipped = flip(pos_flip, (here, got_here, away0, away1), 384)
            by_x = [cut(flipped, x, 2 * rows, 0), swap_row(cut(flipped, 1 - x, 2 * rows, 0), X_BIT)]
            s_all = []
            for f in by_x:
                s_all += [cut(f, c, rows, 0), swap_row(cut(f, 1 - c, rows, 0), CORE_BIT)]
            s_all = jnp.stack(s_all)
            mixed = fold(pos_fold, mix_own, mix_oth, s_all, occ_l, vir_l, n_occ, n_vir)

            def close(n):
                _, home, got = terms[n]
                return finish(n, pos_fold, oovv_block, home, got, mixed, d_block, F32 if last else BF16)

            for n in range(N_CHUNK):
                if terms[n] is None:
                    terms[n] = ladder_part(n)
            return [close(n) for n in range(N_CHUNK)]

        mid = sweep(t_first, [near_half(p) for p in t_first], False)
        final = sweep([p[0] for p in mid], [p[1] for p in mid], True)
        return join_cols([p[0] for p in final])

    return jax.shard_map(
        local_sweeps,
        mesh=mesh,
        in_specs=(blk_spec, blk_spec, blk_spec, blk_spec, P(), P(None, "col")),
        out_specs=blk_spec,
        check_vma=False,
    )
```
